32 devices in a mesh: owner: 8 (over z, core), sub: 4 (over y, x).
Axes of the slice: x: 2, y: 2, z: 4, core: 2. Of those that a mesh axis runs over, the one named last changes fastest.
Arguments:
- residual: float32 [256, 4608], P('owner', 'sub'), may hold values from -6 to 6
- counts: int32 [8, 16], P('owner', 'sub'), may hold values from 1 to 36
- assembly: int32 [8, 16, 36, 2304], P('owner', 'sub'), may hold values from 0 to 1, as said below
- level_two: float32 [8, 2304, 2304], P('owner', 'sub'), as said below
- block_inverse: float32 [8, 2304, 144], P('owner', 'sub'), as said below
Outputs:
- corrections: float32 [256, 4608], P('owner', 'sub')
- level_residual: float32 [8, 2304, 256], P('owner', 'sub')
The draws below stay inside these ranges and needn't reach their ends.
Inputs may be any that keep to these rules, and one draw needn't show every extreme that they name: `assembly`: every row of each [36, 2304] block holds exactly one 1; split the 2304 columns into 4 equal ranges and a group's positions into runs of 4: the 144 rows of one run (live or not) put at most 72 of their 1s into one range, and in every run some range gets exactly 72. `level_two`: each group's matrix is symmetric positive definite. `block_inverse`: each diagonal block is symmetric positive definite.
All inputs are finite; a program needn't handle non-finite values.
Results may differ from the reference program's by a relative error of at most 0.0003.
Values sent between devices are 32-bit elements; how exact they have to be, the bound alone decides.
A program may use at most 64 MiB of HBM per device.

```python
import math
import jax
import jax.numpy as jnp
from jax import lax

PRIM = 36
NC = 2304
BLOCK = 144
ITERS = 4
SUB_DEV = 4
RHS = 256
GSUBS = 16
GROUPS = 8
SUBS = 128
ROUTE = 72
N_OWNER = 8
N_SUB = 4


def one_run(key):
    rows = SUB_DEV * PRIM
    held = NC // N_SUB
    key_a, key_b, key_c, key_d = jax.random.split(key, 4)
    first = jax.random.randint(key_a, (), 0, N_SUB).astype(jnp.int32)
    others = jax.random.permutation(key_b, (N_SUB - 1) * ROUTE).astype(jnp.int32)
    other_holder = others // ROUTE
    other_holder = other_holder + (other_holder >= first).astype(jnp.int32)
    holders = jnp.concatenate([jnp.zeros((ROUTE,), jnp.int32) + first, other_holder[:rows - ROUTE]])
    holders = jax.random.permutation(key_c, holders)
    offsets = jax.random.randint(key_d, (rows,), 0, held).astype(jnp.int32)
    return holders * held + offsets


def draw_assembly(key, part):
    keys = jax.random.split(jax.random.fold_in(key, 11), GROUPS * N_SUB)
    picks = jax.vmap(one_run)(keys).reshape(GROUPS, GSUBS, PRIM)
    columns = lax.broadcasted_iota(jnp.int32, (GROUPS, GSUBS, PRIM, NC), 3)
    return (columns == picks[..., None]).astype(jnp.int32)


def one_matrix(key):
    key_a, key_b, key_c = jax.random.split(key, 3)
    noise = jax.random.normal(key_a, (NC, NC), jnp.float32)
    eye = jnp.eye(NC, dtype=jnp.float32)
    off = (noise + noise.T) * (0.5 / math.sqrt(NC)) * (1.0 - eye)
    rowsum = jnp.sum(jnp.abs(off), axis=1)
    lift = jax.random.uniform(key_b, (NC,), jnp.float32, 0.05, 1.0) * jnp.mean(rowsum)
    diag = 1.25 * rowsum + lift
    matrix = (off + diag[:, None] * eye) / jnp.mean(diag)
    return matrix


def draw_level_two(key, part):
    keys = jax.random.split(jax.random.fold_in(key, 23), GROUPS)
    return lax.map(one_matrix, keys)


def draw_block_inverse(key, part):
    nblocks = NC // BLOCK
    key_a, key_b = jax.random.split(jax.random.fold_in(key, 37))
    noise = jax.random.uniform(key_a, (GROUPS, nblocks, BLOCK, BLOCK), jnp.float32, -1.0, 1.0)
    eye = jnp.eye(BLOCK, dtype=jnp.float32)
    off = (noise + jnp.swapaxes(noise, 2, 3)) * (0.2 / BLOCK) * (1.0 - eye)
    diag = jnp.exp(jax.random.uniform(key_b, (GROUPS, nblocks, BLOCK), jnp.float32, -0.7, 0.7))
    blocks = off + diag[..., None] * eye
    return blocks.reshape(GROUPS, NC, BLOCK)


def with_ends(values, key, low, largest):
    extent = values.shape
    spot = [jax.random.randint(jax.random.fold_in(key, axis), (), 0, extent[axis]) for axis in range(len(extent))]
    values = values.at[tuple(spot)].set(low)
    longest = extent.index(max(extent))
    spot[longest] = (spot[longest] + 1) % extent[longest]
    return values.at[tuple(spot)].set(largest)


def block_scale(own_key, extent, cuts, smallest, largest):
    gain, own = 1.0, jax.random.fold_in(own_key, 6)
    for position, shards_of in cuts:
        steps = jnp.exp(jax.random.uniform(jax.random.fold_in(own, position), (shards_of,), jnp.float32, smallest / len(cuts), largest / len(cuts)))
        gain = gain * jnp.repeat(steps, extent[position] // shards_of).reshape([-1 if axis == position else 1 for axis in range(len(extent))])
    return gain


def gaussian(own_key, shape, width, most, shards=(), kind=jnp.bfloat16):
    array = width * jax.random.normal(own_key, shape, jnp.float32)
    if shards:
        array = array * block_scale(own_key, shape, shards, -0.22, 0.18)
    return jnp.clip(array, -most, most).astype(kind)


def setup_inputs(seed: int = 0) -> dict:
    key_list = jax.random.split(jax.random.key(seed), 6)
    return {
        "residual": gaussian(key_list[0], (RHS, SUBS * PRIM), 1.0, 6.0, ((0, 8), (1, 4)), jnp.float32),
        "counts": with_ends(jax.random.randint(key_list[1], (GROUPS, GSUBS), 1, PRIM + 1), jax.random.fold_in(key_list[1], 1), 1, PRIM).astype(jnp.int32),
        "assembly": draw_assembly(jax.random.fold_in(key_list[5], 71), 0),
        "level_two": draw_level_two(jax.random.fold_in(key_list[5], 71), 0),
        "block_inverse": draw_block_inverse(jax.random.fold_in(key_list[5], 71), 0),
    }


def precondition(inverse, vector):
    nblocks = NC // BLOCK
    blocks = inverse.reshape(nblocks, BLOCK, BLOCK)
    shaped = vector.reshape(nblocks, BLOCK, RHS)
    return jnp.einsum("bij,bjr->bir", blocks, shaped, precision=lax.Precision.HIGHEST).reshape(NC, RHS)


def solve_group(items):
    local, count_row, blocks, matrix, inverse = items
    live = (lax.broadcasted_iota(jnp.int32, (GSUBS, PRIM), 1) < count_row[:, None]).astype(jnp.float32)
    basis = blocks.reshape(GSUBS * PRIM, NC).astype(jnp.float32) * live.reshape(GSUBS * PRIM)[:, None]
    rhs = jnp.dot(basis.T, local, precision=lax.Precision.HIGHEST, preferred_element_type=jnp.float32)
    solution = jnp.zeros((NC, RHS), jnp.float32)
    resid = rhs
    zvec = precondition(inverse, resid)
    direction = zvec
    rz_now = jnp.sum(resid * zvec, axis=0)
    for step in range(ITERS):
        image = jnp.dot(matrix, direction, precision=lax.Precision.HIGHEST, preferred_element_type=jnp.float32)
        alpha = rz_now / jnp.sum(direction * image, axis=0)
        solution = solution + alpha * direction
        resid = resid - alpha * image
        zvec = precondition(inverse, resid)
        rz_next = jnp.sum(resid * zvec, axis=0)
        direction = zvec + (rz_next / rz_now) * direction
        rz_now = rz_next
    corr = jnp.dot(basis, solution, precision=lax.Precision.HIGHEST, preferred_element_type=jnp.float32)
    return corr, resid


def reference(residual, counts, assembly, level_two, block_inverse):
    shaped = residual.reshape(RHS, N_SUB, N_OWNER, SUB_DEV, PRIM)
    local = jnp.transpose(shaped, (2, 1, 3, 4, 0)).reshape(N_OWNER, GSUBS * PRIM, RHS)
    corr, resid = lax.map(solve_group, (local, counts, assembly, level_two, block_inverse))
    back = corr.reshape(N_OWNER, N_SUB, SUB_DEV, PRIM, RHS)
    corrections = jnp.transpose(back, (4, 1, 0, 2, 3)).reshape(RHS, SUBS * PRIM)
    return corrections, resid
```

```python
import functools

import jax
import jax.numpy as jnp
from jax import lax
from jax.experimental import pallas as pl
from jax.experimental.pallas import tpu as pltpu
from jax.sharding import PartitionSpec as P

ITERS = 4
LANES = 128
MESH = pl.DeviceIdType.MESH
F32 = jnp.float32
BF16 = jnp.bfloat16


def split(value):
    high = value.astype(BF16)
    return high, (value - high.astype(F32)).astype(BF16)


def split_cat(value):
    return jnp.concatenate(split(value), axis=1)


def fold(value):
    return value[:, :LANES] + value[:, LANES:]


def rows8(value):
    return jnp.sum(value.reshape(value.shape[0] // 8, 8, value.shape[1]), axis=0)


def dot(left, right):
    return jnp.dot(left, right, preferred_element_type=F32)


def total(acc):
    return jnp.sum(acc, axis=0, keepdims=True)


def iota(shape, axis):
    return lax.broadcasted_iota(jnp.int32, shape, axis)


def piece_dims(local, quota):
    wide = local - local % LANES
    rest = local % LANES
    return wide, rest, quota + (8 if rest else 0)


def kernel(
    dims,
    res_hbm,
    counts_ref,
    hot_hbm,
    inv_hbm,
    mat_hbm,
    corr_out,
    resid_out,
    res,
    mat,
    mat_hi,
    mat_lo,
    zcat,
    rvec,
    zloc,
    ploc,
    wbuf,
    wlast,
    inv_own,
    inv_pack,
    inv_hi,
    inv_lo,
    tbuf,
    trow,
    send_pieces,
    recv_pieces,
    lbuf,
    lcat,
    hotmat,
    pick,
    ypick,
    corr,
    pw_buf,
    corr_pieces,
    corr_back,
    hot_own,
    tcol,
    res_sem,
    mat_sem,
    inv_sem,
    hot_sem,
    sub_send,
    sub_recv,
    small_send,
    small_recv,
    own_send,
    own_recv,
):
    no, ns, rows, width, block, local, rhs = dims
    chunks = rhs // LANES
    nblk = width // block
    per = rows // block
    quota = rhs // no
    half = block // 2
    wide, rest, slab = piece_dims(local, quota)
    parts = LANES // quota
    mo = lax.axis_index("owner")
    me = lax.axis_index("sub")
    relay = ns == 4
    xn = me + 1 - 2 * lax.rem(me, 2)
    yn = lax.rem(me + 2, ns)
    far = 3 - me
    pending = []

    def at(ref, start, size):
        return ref.at[pl.ds(pl.multiple_of(start, 8), size)]

    def span(start, size):
        return pl.ds(pl.multiple_of(start, 8), size)

    def remote(src, dst, ssem, rsem, where):
        return pltpu.make_async_remote_copy(
            src_ref=src, dst_ref=dst, send_sem=ssem, recv_sem=rsem, device_id=where,
            device_id_type=MESH,
        )

    res_copy = pltpu.make_async_copy(res_hbm, res, res_sem)
    hot_copy = pltpu.make_async_copy(hot_hbm.at[0], hot_own, hot_sem)
    inv_copy = pltpu.make_async_copy(inv_hbm.at[0], inv_own, inv_sem)
    mat_copy = pltpu.make_async_copy(mat_hbm.at[0], mat, mat_sem)
    res_copy.start()
    hot_copy.start()
    inv_copy.start()
    mat_copy.start()

    barrier = pltpu.get_barrier_semaphore()
    for step in range(1, ns):
        pl.semaphore_signal(
            barrier, inc=1, device_id={"sub": lax.rem(me + step, ns)}, device_id_type=MESH
        )
    for step in range(1, no):
        pl.semaphore_signal(
            barrier, inc=1, device_id={"owner": lax.rem(mo + step, no)}, device_id_type=MESH
        )

    class Gather:
        def __init__(self, index, buf, size):
            self.index, self.buf, self.size = index, buf, size
            self.cut = (size // 2 + 7) // 8 * 8
            self.copies = []
            self.sent_on = False

        def part(self, who, part):
            if part == 0:
                return at(self.buf, who * self.size, self.cut)
            return at(self.buf, who * self.size + self.cut, self.size - self.cut)

        def add(self, kind, piece, peer):
            copy = remote(
                piece, piece, sub_send.at[self.index, kind], sub_recv.at[self.index, kind],
                {"sub": peer},
            )
            copy.start()
            self.copies.append(copy)
            pending.append(copy)

        def start(self):
            if relay:
                for kind, (peer, part) in enumerate(((xn, 0), (yn, 1), (xn, 1), (yn, 0))):
                    self.add(kind, self.part(me, part), peer)
            else:
                mine = at(self.buf, me * self.size, self.size)
                for step in range(1, ns):
                    self.add(step - 1, mine, lax.rem(me + step, ns))

        def forward(self):
            if relay and not self.sent_on:
                self.copies[0].wait_recv()
                self.add(4, self.part(xn, 0), yn)
                self.copies[1].wait_recv()
                self.add(5, self.part(yn, 1), xn)
            self.sent_on = True

        def pieces(self):
            size, cut = self.size, self.cut
            if relay:
                return [
                    (None, xn * size, cut),
                    (None, yn * size + cut, size - cut),
                    (self.copies[2], xn * size + cut, size - cut),
                    (self.copies[3], yn * size, cut),
                    (self.copies[4], far * size, cut),
                    (self.copies[5], far * size + cut, size - cut),
                ]
            return [
                (self.copies[step - 1], lax.rem(me + ns - step, ns) * size, size)
                for step in range(1, ns)
            ]

        def finish(self):
            self.forward()
            for copy, _, _ in self.pieces():
                if copy is not None:
                    copy.wait_recv()

    def small_gather(index, buf, size):
        copies = []
        for step in range(1, ns):
            mine = at(buf, me * size, size)
            copy = remote(
                mine, mine, small_send.at[index, step - 1], small_recv.at[index, step - 1],
                {"sub": lax.rem(me + step, ns)},
            )
            copy.start()
            copies.append(copy)
            pending.append(copy)
        return copies

    def owner_copy(index, src, dst, peer):
        return remote(
            at(src, peer * slab, slab), at(dst, mo * slab, slab),
            own_send.at[index, peer], own_recv.at[index, mo], {"owner": peer},
        )

    def owner_wait(index, dst, peer):
        @pl.when(mo != peer)
        def _():
            piece = at(dst, peer * slab, slab)
            remote(
                piece, piece, own_send.at[index, peer], own_recv.at[index, peer],
                {"owner": peer},
            ).wait_recv()

    hot_copy.wait()
    prim, slots = hot_own.shape[0], hot_own.shape[1]
    for q in range(slots):
        acc = jnp.zeros((prim, LANES), F32)
        spot = iota((prim, LANES), 1)
        for lane in range(0, width, LANES):
            acc += (hot_own[:, q, lane : lane + LANES] * (spot + lane)).astype(F32)
        value = jnp.sum(acc, axis=1, keepdims=True)
        alive = iota((prim, 1), 0) < counts_ref[0, q]
        tcol[q * prim : (q + 1) * prim, :] = jnp.broadcast_to(
            jnp.where(alive, value, -1.0), (prim, LANES)
        )
    tbuf[span(me * 8, 8), :] = tcol[...].T[:8, :]

    res_copy.wait()
    for part in range(no):
        low = part * local
        send_pieces[part * slab : part * slab + quota, :] = res[:, low : low + wide]
        if rest:
            strips = [
                res[t : t + 8, low + wide : low + local] for t in range(0, quota, 8)
            ]
            strips.append(jnp.zeros((8, wide - rest * len(strips)), F32))
            send_pieces[part * slab + quota : (part + 1) * slab, :] = jnp.concatenate(
                strips, axis=1
            )

    pl.semaphore_wait(barrier, ns - 1 + no - 1)

    for step in range(1, no):
        copy = owner_copy(0, send_pieces, recv_pieces, lax.rem(mo + step, no))
        copy.start()
        pending.append(copy)
    targets = small_gather(0, tbuf, 8)
    recv_pieces[span(mo * slab, slab), :] = send_pieces[span(mo * slab, slab), :]

    inv_copy.wait()
    prow, pcol = iota((half, block), 0), iota((half, block), 1)
    segments, diagonals = [], []
    for q in range(per):
        top = inv_own[:half, q * block : (q + 1) * block]
        last = jnp.concatenate(
            [
                inv_own[half:block, q * block + half : (q + 1) * block],
                jnp.zeros((half, block - half), F32),
            ],
            axis=1,
        )
        segments.append(jnp.where(pcol >= prow, top, last))
        diagonals.append(jnp.sum(jnp.where(pcol == prow, last, 0.0), axis=1, keepdims=True))
    pad = inv_pack.shape[1] - rows - per
    inv_pack[span(me * half, half), :] = jnp.concatenate(
        segments + diagonals + [jnp.zeros((half, pad), F32)], axis=1
    )
    inv_gather = Gather(0, inv_pack, half)
    inv_gather.start()

    mat_copy.wait()
    strip = 48

    @pl.loop(0, rows // strip)
    def _(t):
        here = span(t * strip, strip)
        high, low = split(mat[here, :])
        mat_hi[here, :] = high
        mat_lo[here, :] = low

    inv_gather.forward()

    local_gathers = []
    for c in range(chunks):
        owners = range(c * parts, (c + 1) * parts)
        for o in owners:
            owner_wait(0, recv_pieces, o)
        body = jnp.concatenate(
            [recv_pieces[o * slab : o * slab + quota, :] for o in owners], axis=0
        )
        lbuf[c, span(me * local, wide), :] = body.T
        if rest:
            ends = jnp.concatenate(
                [
                    recv_pieces[o * slab + quota : (o + 1) * slab, t * rest : (t + 1) * rest]
                    for o in owners
                    for t in range(quota // 8)
                ],
                axis=0,
            )
            lbuf[c, span(me * local + wide, rest), :] = ends.T
        gather = Gather(1 + c, lbuf.at[c], local)
        gather.start()
        local_gathers.append(gather)

    for lane in range(0, width, 2 * LANES):
        spot = iota((local, 2 * LANES), 1).astype(F32) + float(lane)
        pick[:, lane : lane + 2 * LANES] = jnp.where(spot == tcol[:, :1], 1.0, 0.0).astype(BF16)

    for copy in targets:
        copy.wait_recv()
    trow[...] = jnp.broadcast_to(
        jnp.concatenate([tbuf[s * 8 : s * 8 + 1, :] for s in range(ns)], axis=1), trow.shape
    )

    @pl.loop(0, width // strip)
    def _(t):
        spot = (iota((strip, ns * local), 0) + t * strip).astype(F32)
        hotmat[span(t * strip, strip), :] = jnp.where(spot == trow[:1, :], 1.0, 0.0).astype(BF16)

    local_gathers[0].forward()
    inv_gather.finish()

    @pl.loop(0, ns)
    def _(s):
        packed = inv_pack.at[span(s * half, half)]
        brow, bcol = iota((block, block), 0), iota((block, block), 1)
        for q in range(per):
            segment = packed[:, q * block : (q + 1) * block]
            ends = packed[:, rows + q : rows + q + 1]
            top = jnp.where(pcol >= prow, segment, 0.0)
            last = jnp.where(pcol < prow, segment, jnp.where(pcol == prow, ends, 0.0))
            low = jnp.concatenate(
                [jnp.zeros((half, half), F32), last[:, : block - half]], axis=1
            )
            one = jnp.concatenate([top, low], axis=0)
            high, low = split(jnp.where(brow == bcol, one, one + one.T))
            inv_hi[s * per + q] = high
            inv_lo[s * per + q] = low

    for gather in local_gathers[1:]:
        gather.forward()

    def precond(b, resid):
        rcat = split_cat(resid)
        return fold(dot(inv_hi[b], rcat) + dot(inv_lo[b], rcat))

    def first(c):
        lcat[...] = split_cat(lbuf[c])

        def one(b):
            here = span(b * block, block)
            resid = fold(dot(hotmat[here, :], lcat[...]))
            rvec[c, here, :] = resid
            z = precond(b, resid)
            zcat[c, here, :] = split_cat(z)
            return z, rows8(resid * z)

        acc = jnp.zeros((8, LANES), F32)
        for q in range(per):
            z, part = one(me * per + q)
            zloc[c, q * block : (q + 1) * block, :] = z
            acc = acc + part
        group = 4 if (nblk - per) % 4 == 0 else 3 if (nblk - per) % 3 == 0 else 1

        def step(t, acc):
            for u in range(group):
                acc = acc + one(lax.rem(me * per + per + t * group + u, nblk))[1]
            return acc

        return total(lax.fori_loop(0, (nblk - per) // group, step, acc))

    def update(k, c, gather, sums, rz):
        for copy in sums:
            copy.wait_recv()
        alpha = rz / total(rows8(pw_buf[k, c]))
        corr[c] = alpha * ypick[c] + (corr[c] if k else 0.0)

        def one(b):
            here = span(b * block, block)
            resid = rvec[c, here, :] - alpha * wbuf[k, c, here, :]
            rvec[c, here, :] = resid
            z = precond(b, resid)
            zcat[c, here, :] = split_cat(z)
            return z, rows8(resid * z)

        acc = jnp.zeros((8, LANES), F32)
        for q in range(per):
            z, part = one(me * per + q)
            zloc[c, q * block : (q + 1) * block, :] = z
            acc = acc + part
        gather.forward()
        for copy, start, size in gather.pieces():
            if copy is not None:
                copy.wait_recv()
            for u in range(size // block):
                acc = acc + one(start // block + u)[1]
        rz_next = total(acc)
        return rz_next, rz_next / rz

    tile = 2 * block if rows % (2 * block) == 0 else block

    def image(k, c, beta):
        def body(t, acc):
            here = span(t * tile, tile)
            there = span(me * rows + t * tile, tile)
            w = fold(dot(mat_hi[here, :], zcat[c]) + dot(mat_lo[here, :], zcat[c]))
            p = zloc[c, here, :]
            if k:
                w = w + beta * wbuf[k - 1, c, there, :]
                p = p + beta * ploc[c, here, :]
            ploc[c, here, :] = p
            if k < ITERS - 1:
                wbuf[k, c, there, :] = w
            else:
                wlast[c, here, :] = w
            return acc + rows8(p * w)

        acc = lax.fori_loop(0, rows // tile, body, jnp.zeros((8, LANES), F32))
        pw_buf[k, c, span(me * 8, 8), :] = acc
        return small_gather(1 + k * chunks + c, pw_buf.at[k, c], 8)

    def spread(k, c, earlier):
        if earlier is not None:
            earlier.forward()
        gather = Gather(1 + chunks + k * chunks + c, wbuf.at[k, c], rows)
        gather.start()
        return gather

    def picked(k, c, beta):
        y = fold(dot(pick[...], zcat[c]))
        ypick[c] = y + beta * ypick[c] if k else y

    def conclude(c, sums, rz):
        for copy in sums:
            copy.wait_recv()
        alpha = rz / total(rows8(pw_buf[ITERS - 1, c]))
        value = corr[c] + alpha * ypick[c]
        owners = range(c * parts, (c + 1) * parts)
        body = value[:wide, :].T
        ends = value[wide:, :].T if rest else None
        for o in owners:
            low = (o - c * parts) * quota
            corr_pieces[o * slab : o * slab + quota, :] = body[low : low + quota, :]
            if rest:
                strips = [ends[low + t : low + t + 8, :] for t in range(0, quota, 8)]
                strips.append(jnp.zeros((8, wide - rest * len(strips)), F32))
                corr_pieces[o * slab + quota : (o + 1) * slab, :] = jnp.concatenate(
                    strips, axis=1
                )
        for o in owners:
            @pl.when(mo != o)
            def _(o=o):
                owner_copy(1, corr_pieces, corr_back, o).start()
        resid_out[0, :, c * LANES : (c + 1) * LANES] = (
            rvec[c, span(me * rows, rows), :] - alpha * wlast[c]
        )

    rz, beta = [None] * chunks, [None] * chunks
    sums, flight, earlier = [None] * chunks, [None] * chunks, None
    for c in range(chunks):
        local_gathers[c].finish()
        rz[c] = first(c)
        sums[c] = image(0, c, None)
        earlier = flight[c] = spread(0, c, earlier)
        picked(0, c, None)

    for k in range(ITERS - 1):
        final = k == ITERS - 2
        for c in range(chunks):
            if final and c:
                earlier.forward()
                conclude(c - 1, sums[c - 1], rz[c - 1])
            rz[c], beta[c] = update(k, c, flight[c], sums[c], rz[c])
            sums[c] = image(k + 1, c, beta[c])
            if not final:
                earlier = flight[c] = spread(k + 1, c, earlier)
            picked(k + 1, c, beta[c])
    conclude(chunks - 1, sums[-1], rz[-1])

    corr_back[span(mo * slab, slab), :] = corr_pieces[span(mo * slab, slab), :]
    for part in range(no):
        owner_wait(1, corr_back, part)
        low = part * local
        corr_out[:, low : low + wide] = corr_back[part * slab : part * slab + quota, :]
        for t in range(quota // 8 if rest else 0):
            corr_out[8 * t : 8 * t + 8, low + wide : low + local] = corr_back[
                part * slab + quota : (part + 1) * slab, t * rest : (t + 1) * rest
            ]
    for copy in pending:
        copy.wait_send()
    for o in range(no):
        @pl.when(mo != o)
        def _(o=o):
            owner_copy(1, corr_pieces, corr_back, o).wait_send()


def shards(no, ns, residual, counts, assembly, level_two, block_inverse):
    _, slots, prim, width = assembly.shape
    rows = level_two.shape[1]
    block = block_inverse.shape[2]
    local = slots * prim
    quota = residual.shape[0]
    rhs = quota * no
    chunks = rhs // LANES
    nblk = width // block
    per = rows // block
    half = block // 2
    wide, _, slab = piece_dims(local, quota)
    packed = pl.cdiv(rows + per, LANES) * LANES
    kinds = 6 if ns == 4 else ns - 1
    vmem = pl.BlockSpec(memory_space=pltpu.VMEM)
    anywhere = pl.BlockSpec(memory_space=pl.ANY)
    dma = pltpu.SemaphoreType.DMA
    dims = (no, ns, rows, width, block, local, rhs)
    return pl.pallas_call(
        functools.partial(kernel, dims),
        out_shape=(pltpu.VMEM(residual.shape, F32), pltpu.VMEM((1, rows, rhs), F32)),
        in_specs=[anywhere, pl.BlockSpec(memory_space=pltpu.SMEM)] + [anywhere] * 3,
        out_specs=(vmem, vmem),
        scratch_shapes=[
            pltpu.VMEM(residual.shape, F32),
            pltpu.VMEM((rows, width), F32),
            pltpu.VMEM((rows, width), BF16),
            pltpu.VMEM((rows, width), BF16),
            pltpu.VMEM((chunks, width, 2 * LANES), BF16),
            pltpu.VMEM((chunks, width, LANES), F32),
            pltpu.VMEM((chunks, rows, LANES), F32),
            pltpu.VMEM((chunks, rows, LANES), F32),
            pltpu.VMEM((ITERS - 1, chunks, width, LANES), F32),
            pltpu.VMEM((chunks, rows, LANES), F32),
            pltpu.VMEM((block, rows), F32),
            pltpu.VMEM((ns * half, packed), F32),
            pltpu.VMEM((nblk, block, block), BF16),
            pltpu.VMEM((nblk, block, block), BF16),
            pltpu.VMEM((ns * 8, local), F32),
            pltpu.VMEM((8, ns * local), F32),
            pltpu.VMEM((no * slab, wide), F32),
            pltpu.VMEM((no * slab, wide), F32),
            pltpu.VMEM((chunks, ns * local, LANES), F32),
            pltpu.VMEM((ns * local, 2 * LANES), BF16),
            pltpu.VMEM((width, ns * local), BF16),
            pltpu.VMEM((local, width), BF16),
            pltpu.VMEM((chunks, local, LANES), F32),
            pltpu.VMEM((chunks, local, LANES), F32),
            pltpu.VMEM((ITERS, chunks, ns * 8, LANES), F32),
            pltpu.VMEM((no * slab, wide), F32),
            pltpu.VMEM((no * slab, wide), F32),
            pltpu.VMEM((prim, slots, width), jnp.int32),
            pltpu.VMEM((local, LANES), F32),
            dma,
            dma,
            dma,
            dma,
            dma((1 + ITERS * chunks, kinds)),
            dma((1 + ITERS * chunks, kinds)),
            dma((1 + ITERS * chunks, ns - 1)),
            dma((1 + ITERS * chunks, ns - 1)),
            dma((2, no)),
            dma((2, no)),
        ],
        compiler_params=pltpu.CompilerParams(
            collective_id=0, has_side_effects=True, vmem_limit_bytes=60 * 1024 * 1024
        ),
    )(
        residual,
        counts,
        jnp.swapaxes(assembly, 1, 2),
        jnp.swapaxes(block_inverse, 1, 2),
        level_two,
    )


def solution(mesh):
    in_specs = (
        P("owner", "sub"),
        P("owner", "sub"),
        P("owner", "sub", None, None),
        P("owner", "sub", None),
        P("owner", "sub", None),
    )
    out_specs = (P("owner", "sub"), P("owner", "sub", None))
    body = functools.partial(shards, mesh.shape["owner"], mesh.shape["sub"])
    return jax.shard_map(body, mesh=mesh, in_specs=in_specs, out_specs=out_specs, check_vma=False)
```

```python
import functools

import jax
import jax.numpy as jnp
from jax import lax
from jax.experimental import pallas as pl
from jax.experimental.pallas import tpu as pltpu
from jax.sharding import PartitionSpec as P

ITERS = 4
LANES = 128
MESH = pl.DeviceIdType.MESH
F32 = jnp.float32
BF16 = jnp.bfloat16


def split(value):
    high = value.astype(BF16)
    return high, (value - high.astype(F32)).astype(BF16)


def split_cat(value):
    return jnp.concatenate(split(value), axis=1)


def fold(value):
    return value[:, :LANES] + value[:, LANES:]


def rows8(value):
    return jnp.sum(value.reshape(value.shape[0] // 8, 8, value.shape[1]), axis=0)


def dot(left, right):
    return jnp.dot(left, right, preferred_element_type=F32)


def total(acc):
    return jnp.sum(acc, axis=0, keepdims=True)


def iota(shape, axis):
    return lax.broadcasted_iota(jnp.int32, shape, axis)


def chunk_owners(chunks, parts, c):
    if chunks != 2 or parts % 2:
        return list(range(c * parts, (c + 1) * parts))
    side = parts // 2
    return [t * side + u for t in ((0, 2), (3, 1))[c] for u in range(side)]


def piece_dims(local, quota):
    wide = local - local % LANES
    rest = local % LANES
    return wide, rest, quota + (8 if rest else 0)


def kernel(
    dims,
    res_hbm,
    counts_ref,
    hot_hbm,
    inv_hbm,
    mat_hbm,
    corr_out,
    resid_out,
    res,
    mat,
    mat_hi,
    mat_lo,
    zcat,
    rvec,
    zloc,
    ploc,
    wbuf,
    wlast,
    inv_own,
    inv_pack,
    inv_hi,
    inv_lo,
    tbuf,
    send_pieces,
    recv_pieces,
    lbuf,
    lcat,
    hotmat,
    pick,
    ypick,
    corr,
    pw_buf,
    corr_pieces,
    corr_back,
    hot_own,
    tcol,
    res_sem,
    mat_sem,
    inv_sem,
    hot_sem,
    sub_send,
    sub_recv,
    small_send,
    small_recv,
    own_send,
    own_recv,
):
    no, ns, rows, width, block, local, rhs = dims
    chunks = rhs // LANES
    nblk = width // block
    per = rows // block
    quota = rhs // no
    half = block // 2
    wide, rest, slab = piece_dims(local, quota)
    parts = LANES // quota
    mo = lax.axis_index("owner")
    me = lax.axis_index("sub")
    relay = ns == 4
    xn = me + 1 - 2 * lax.rem(me, 2)
    yn = lax.rem(me + 2, ns)
    far = 3 - me
    pending = []

    def at(ref, start, size):
        return ref.at[pl.ds(pl.multiple_of(start, 8), size)]

    def span(start, size):
        return pl.ds(pl.multiple_of(start, 8), size)

    def remote(src, dst, ssem, rsem, where):
        return pltpu.make_async_remote_copy(
            src_ref=src, dst_ref=dst, send_sem=ssem, recv_sem=rsem, device_id=where,
            device_id_type=MESH,
        )

    res_copy = pltpu.make_async_copy(res_hbm, res, res_sem)
    hot_copy = pltpu.make_async_copy(hot_hbm.at[0], hot_own, hot_sem)
    inv_copy = pltpu.make_async_copy(inv_hbm.at[0], inv_own, inv_sem)
    mat_copy = pltpu.make_async_copy(mat_hbm.at[0], mat, mat_sem)
    res_copy.start()
    hot_copy.start()
    inv_copy.start()
    mat_copy.start()

    barrier = pltpu.get_barrier_semaphore()
    for step in range(1, ns):
        pl.semaphore_signal(
            barrier, inc=1, device_id={"sub": lax.rem(me + step, ns)}, device_id_type=MESH
        )
    for step in range(1, no):
        pl.semaphore_signal(
            barrier, inc=1, device_id={"owner": lax.rem(mo + step, no)}, device_id_type=MESH
        )

    class Gather:
        def __init__(self, index, buf, size):
            self.index, self.buf, self.size = index, buf, size
            self.cut = (size // 2 + 7) // 8 * 8
            self.copies = {}
            self.sent_on = False

        def part(self, who, part):
            if part == 0:
                return at(self.buf, who * self.size, self.cut)
            return at(self.buf, who * self.size + self.cut, self.size - self.cut)

        def add(self, kind, piece, peer):
            copy = remote(
                piece, piece, sub_send.at[self.index, kind], sub_recv.at[self.index, kind],
                {"sub": peer},
            )
            copy.start()
            self.copies[kind] = copy
            pending.append(copy)

        def start_part(self, part):
            for kind in ((0, 3), (1, 2))[part]:
                self.add(kind, self.part(me, part), xn if kind in (0, 2) else yn)

        def start(self):
            if relay:
                for kind, (peer, part) in enumerate(((xn, 0), (yn, 1), (xn, 1), (yn, 0))):
                    self.add(kind, self.part(me, part), peer)
            else:
                mine = at(self.buf, me * self.size, self.size)
                for step in range(1, ns):
                    self.add(step - 1, mine, lax.rem(me + step, ns))

        def forward(self):
            if relay and not self.sent_on:
                self.copies[0].wait_recv()
                self.add(4, self.part(xn, 0), yn)
                self.copies[1].wait_recv()
                self.add(5, self.part(yn, 1), xn)
            self.sent_on = True

        def pieces(self):
            size, cut = self.size, self.cut
            if relay:
                return [
                    (None, xn * size, cut),
                    (None, yn * size + cut, size - cut),
                    (self.copies[2], xn * size + cut, size - cut),
                    (self.copies[3], yn * size, cut),
                    (self.copies[4], far * size, cut),
                    (self.copies[5], far * size + cut, size - cut),
                ]
            return [
                (self.copies[step - 1], lax.rem(me + ns - step, ns) * size, size)
                for step in range(1, ns)
            ]

        def runs(self):
            kinds = ((2,), (3,), (4, 5)) if relay else [(step - 1,) for step in range(1, ns)]
            peers = (xn, yn, far) if relay else [lax.rem(me + ns - step, ns) for step in range(1, ns)]
            return list(zip(peers, kinds))

        def finish(self, kinds):
            for kind in kinds:
                self.copies[kind].wait_recv()

    def small_gather(index, buf, size):
        copies = []
        for step in range(1, ns):
            mine = at(buf, me * size, size)
            copy = remote(
                mine, mine, small_send.at[index, step - 1], small_recv.at[index, step - 1],
                {"sub": lax.rem(me + step, ns)},
            )
            copy.start()
            copies.append(copy)
            pending.append(copy)
        return copies

    def owner_copy(index, src, dst, peer):
        return remote(
            at(src, peer * slab, slab), at(dst, mo * slab, slab),
            own_send.at[index, peer], own_recv.at[index, mo], {"owner": peer},
        )

    def owner_wait(index, dst, peer):
        @pl.when(mo != peer)
        def _():
            piece = at(dst, peer * slab, slab)
            remote(
                piece, piece, own_send.at[index, peer], own_recv.at[index, peer],
                {"owner": peer},
            ).wait_recv()

    res_copy.wait()
    for part in range(no):
        low = part * local
        send_pieces[part * slab : part * slab + quota, :] = res[:, low : low + wide]
        if rest:
            strips = [
                res[t : t + 8, low + wide : low + local] for t in range(0, quota, 8)
            ]
            strips.append(jnp.zeros((8, wide - rest * len(strips)), F32))
            send_pieces[part * slab + quota : (part + 1) * slab, :] = jnp.concatenate(
                strips, axis=1
            )

    hot_copy.wait()
    prim, slots = hot_own.shape[0], hot_own.shape[1]
    for q in range(slots):
        acc = jnp.zeros((prim, LANES), F32)
        spot = iota((prim, LANES), 1)
        for lane in range(0, width, LANES):
            acc += (hot_own[:, q, lane : lane + LANES] * (spot + lane)).astype(F32)
        value = jnp.sum(acc, axis=1, keepdims=True)
        alive = iota((prim, 1), 0) < counts_ref[0, q]
        tcol[q * prim : (q + 1) * prim, :] = jnp.broadcast_to(
            jnp.where(alive, value, -1.0), (prim, LANES)
        )
    tbuf[span(me * 8, 8), :] = tcol[...].T[:8, :]

    inv_copy.wait()
    prow, pcol = iota((half, block), 0), iota((half, block), 1)
    segments, diagonals = [], []
    for q in range(per):
        top = inv_own[:half, q * block : (q + 1) * block]
        last = jnp.concatenate(
            [
                inv_own[half:block, q * block + half : (q + 1) * block],
                jnp.zeros((half, block - half), F32),
            ],
            axis=1,
        )
        segments.append(jnp.where(pcol >= prow, top, last))
        diagonals.append(jnp.sum(jnp.where(pcol == prow, last, 0.0), axis=1, keepdims=True))
    pad = inv_pack.shape[1] - rows - per
    inv_pack[span(me * half, half), :] = jnp.concatenate(
        segments + diagonals + [jnp.zeros((half, pad), F32)], axis=1
    )
    pl.semaphore_wait(barrier, ns - 1 + no - 1)

    targets = small_gather(0, tbuf, 8)
    routed = [
        owner_copy(0, send_pieces, recv_pieces, lax.rem(mo + step, no)) for step in range(1, no)
    ]
    pending.extend(routed)
    mixed = chunks == 2 and parts % 2 == 0
    early_owner = lax.rem(mo // (parts // 2), 2) == 0 if mixed else mo >= 0

    @pl.when(early_owner)
    def _():
        for copy in routed:
            copy.start()

    recv_pieces[span(mo * slab, slab), :] = send_pieces[span(mo * slab, slab), :]

    inv_gather = Gather(0, inv_pack, half)
    inv_gather.start()

    mat_copy.wait()
    strip = 48

    @pl.loop(0, rows // strip)
    def _(t):
        here = span(t * strip, strip)
        high, low = split(mat[here, :])
        mat_hi[here, :] = high
        mat_lo[here, :] = low

    @pl.when(jnp.logical_not(early_owner))
    def _():
        for copy in routed:
            copy.start()

    def arrange(c):
        owners = chunk_owners(chunks, parts, c)
        for o in owners:
            owner_wait(0, recv_pieces, o)
        body = jnp.concatenate(
            [recv_pieces[o * slab : o * slab + quota, :] for o in owners], axis=0
        )
        lbuf[c, span(me * local, wide), :] = body.T
        if rest:
            ends = jnp.concatenate(
                [
                    recv_pieces[o * slab + quota : (o + 1) * slab, t * rest : (t + 1) * rest]
                    for o in owners
                    for t in range(quota // 8)
                ],
                axis=0,
            )
            lbuf[c, span(me * local + wide, rest), :] = ends.T
        return Gather(1 + c, lbuf.at[c], local)

    def unpack(s):
        packed = inv_pack.at[span(s * half, half)]
        brow, bcol = iota((block, block), 0), iota((block, block), 1)
        for q in range(per):
            segment = packed[:, q * block : (q + 1) * block]
            ends = packed[:, rows + q : rows + q + 1]
            top = jnp.where(pcol >= prow, segment, 0.0)
            last = jnp.where(pcol < prow, segment, jnp.where(pcol == prow, ends, 0.0))
            low = jnp.concatenate(
                [jnp.zeros((half, half), F32), last[:, : block - half]], axis=1
            )
            one = jnp.concatenate([top, low], axis=0)
            high, low = split(jnp.where(brow == bcol, one, one + one.T))
            inv_hi[s * per + q] = high
            inv_lo[s * per + q] = low

    def seed(c, s, fresh):
        lcat[...] = split_cat(lbuf[c, span(s * local, local), :])

        @pl.loop(0, ns)
        def _(t):
            here = span(t * rows, rows)
            value = fold(dot(hotmat[s, here, :], lcat[...]))
            rvec[c, here, :] = value if fresh else rvec[c, here, :] + value

    unpack(me)
    for lane in range(0, width, 2 * LANES):
        spot = iota((local, 2 * LANES), 1).astype(F32) + float(lane)
        pick[:, lane : lane + 2 * LANES] = jnp.where(spot == tcol[:, :1], 1.0, 0.0).astype(BF16)

    local_gathers = [arrange(0)]
    local_gathers[0].start()
    inv_gather.forward()
    for copy in targets:
        copy.wait_recv()

    @pl.loop(0, ns)
    def _(s):
        goal = tbuf[span(s * 8, 8), :][:1, :]
        for row in range(0, width, block):
            spot = (iota((block, local), 0) + row).astype(F32)
            hotmat[s, row : row + block, :] = jnp.where(spot == goal, 1.0, 0.0).astype(BF16)

    seed(0, me, True)
    inv_runs = inv_gather.runs()
    if relay:
        s, kinds = inv_runs[0]
        inv_gather.finish(kinds)
        unpack(s)
    local_gathers[0].forward()
    if relay:
        s, kinds = inv_runs[1]
        inv_gather.finish(kinds)
        unpack(s)
    for c in range(1, chunks):
        local_gathers.append(arrange(c))
        local_gathers[c].start()
    for s, kinds in local_gathers[0].runs()[:-1]:
        local_gathers[0].finish(kinds)
        seed(0, s, False)
    if relay:
        s, kinds = inv_runs[2]
        inv_gather.finish(kinds)
        unpack(s)
    else:
        for s, kinds in inv_runs:
            inv_gather.finish(kinds)

        @pl.loop(1, ns)
        def _(t):
            unpack(lax.rem(me + t, ns))

    def precond(b, resid):
        rcat = split_cat(resid)
        return fold(dot(inv_hi[b], rcat) + dot(inv_lo[b], rcat))

    def first(c):
        last, kinds = local_gathers[c].runs()[-1]
        local_gathers[c].finish(kinds)
        lcat[...] = split_cat(lbuf[c, span(last * local, local), :])

        def run(s, acc, own):
            value = fold(dot(hotmat[last, span(s * rows, rows), :], lcat[...]))
            value = rvec[c, span(s * rows, rows), :] + value
            rvec[c, span(s * rows, rows), :] = value
            for q in range(per):
                resid = value[q * block : (q + 1) * block, :]
                z = precond(s * per + q, resid)
                zcat[c, span(s * rows + q * block, block), :] = split_cat(z)
                if own:
                    zloc[c, q * block : (q + 1) * block, :] = z
                acc = acc + rows8(resid * z)
            return acc

        acc = run(me, jnp.zeros((8, LANES), F32), True)
        return total(
            lax.fori_loop(1, ns, lambda t, acc: run(lax.rem(me + t, ns), acc, False), acc)
        )

    def update(k, c, gather, sums, rz):
        for copy in sums:
            copy.wait_recv()
        alpha = rz / total(rows8(pw_buf[k, c]))
        corr[c] = alpha * ypick[c] + (corr[c] if k else 0.0)

        def one(b):
            here = span(b * block, block)
            resid = rvec[c, here, :] - alpha * wbuf[k, c, here, :]
            rvec[c, here, :] = resid
            z = precond(b, resid)
            zcat[c, here, :] = split_cat(z)
            return z, rows8(resid * z)

        acc = jnp.zeros((8, LANES), F32)
        for q in range(per):
            z, part = one(me * per + q)
            zloc[c, q * block : (q + 1) * block, :] = z
            acc = acc + part
        gather.forward()
        for copy, start, size in gather.pieces():
            if copy is not None:
                copy.wait_recv()
            for u in range(size // block):
                acc = acc + one(start // block + u)[1]
        rz_next = total(acc)
        return rz_next, rz_next / rz

    tile = 2 * block if rows % (2 * block) == 0 else block

    def image(k, c, beta, gather=None):
        def body(t, acc):
            here = span(t * tile, tile)
            there = span(me * rows + t * tile, tile)
            w = fold(dot(mat_hi[here, :], zcat[c]) + dot(mat_lo[here, :], zcat[c]))
            p = zloc[c, here, :]
            if k:
                w = w + beta * wbuf[k - 1, c, there, :]
                p = p + beta * ploc[c, here, :]
            ploc[c, here, :] = p
            if k < ITERS - 1:
                wbuf[k, c, there, :] = w
            else:
                wlast[c, here, :] = w
            return acc + rows8(p * w)

        acc = jnp.zeros((8, LANES), F32)
        if gather is None:
            acc = lax.fori_loop(0, rows // tile, body, acc)
        else:
            for part in range(2):
                acc = body(part, acc)
                gather.start_part(part)
        pw_buf[k, c, span(me * 8, 8), :] = acc
        return small_gather(1 + k * chunks + c, pw_buf.at[k, c], 8)

    def rows_gather(k, c):
        return Gather(1 + chunks + k * chunks + c, wbuf.at[k, c], rows)

    def spread(k, c, earlier):
        earlier.forward()
        gather = rows_gather(k, c)
        gather.start()
        return gather

    def picked(k, c, beta):
        y = fold(dot(pick[...], zcat[c]))
        ypick[c] = y + beta * ypick[c] if k else y

    def conclude(c, sums, rz):
        for copy in sums:
            copy.wait_recv()
        alpha = rz / total(rows8(pw_buf[ITERS - 1, c]))
        value = corr[c] + alpha * ypick[c]
        owners = chunk_owners(chunks, parts, c)
        body = value[:wide, :].T
        ends = value[wide:, :].T if rest else None
        for t, o in enumerate(owners):
            low = t * quota
            corr_pieces[o * slab : o * slab + quota, :] = body[low : low + quota, :]
            if rest:
                strips = [ends[low + t : low + t + 8, :] for t in range(0, quota, 8)]
                strips.append(jnp.zeros((8, wide - rest * len(strips)), F32))
                corr_pieces[o * slab + quota : (o + 1) * slab, :] = jnp.concatenate(
                    strips, axis=1
                )
        for o in owners:
            @pl.when(mo != o)
            def _(o=o):
                owner_copy(1, corr_pieces, corr_back, o).start()
        left = rvec[c, span(me * rows, rows), :] - alpha * wlast[c]
        if not mixed:
            resid_out[0, :, c * LANES : (c + 1) * LANES] = left
        elif c == 0:
            wlast[c] = left
        else:
            side = iota(left.shape, 1) < LANES // 2
            resid_out[0, :, :LANES] = jnp.where(side, wlast[0], left)
            resid_out[0, :, LANES:] = pltpu.roll(jnp.where(side, left, wlast[0]), LANES // 2, 1)

    rz, beta = [None] * chunks, [None] * chunks
    sums, flight, earlier = [None] * chunks, [None] * chunks, None
    for c in range(chunks):
        if c:
            seed(c, me, True)
            for s, kinds in local_gathers[c].runs()[:-1]:
                local_gathers[c].finish(kinds)
                seed(c, s, False)
        rz[c] = first(c)
        if c == 0:
            for gather in local_gathers[1:]:
                gather.forward()
        if c:
            earlier.forward()
            sums[c] = image(0, c, None)
            earlier = flight[c] = spread(0, c, earlier)
        else:
            earlier = flight[c] = rows_gather(0, c)
            early = relay and tile * 2 == rows and tile == earlier.cut
            sums[c] = image(0, c, None, earlier if early else None)
            if not early:
                earlier.start()
        picked(0, c, None)

    for k in range(ITERS - 1):
        final = k == ITERS - 2
        for c in range(chunks):
            if final and c:
                earlier.forward()
            rz[c], beta[c] = update(k, c, flight[c], sums[c], rz[c])
            sums[c] = image(k + 1, c, beta[c])
            if not final:
                earlier = flight[c] = spread(k + 1, c, earlier)
            picked(k + 1, c, beta[c])
    for c in range(chunks):
        conclude(c, sums[c], rz[c])

    corr_back[span(mo * slab, slab), :] = corr_pieces[span(mo * slab, slab), :]
    for part in range(no):
        owner_wait(1, corr_back, part)
        low = part * local
        corr_out[:, low : low + wide] = corr_back[part * slab : part * slab + quota, :]
        for t in range(quota // 8 if rest else 0):
            corr_out[8 * t : 8 * t + 8, low + wide : low + local] = corr_back[
                part * slab + quota : (part + 1) * slab, t * rest : (t + 1) * rest
            ]
    for copy in pending:
        copy.wait_send()
    for o in range(no):
        @pl.when(mo != o)
        def _(o=o):
            owner_copy(1, corr_pieces, corr_back, o).wait_send()


def shards(no, ns, residual, counts, assembly, level_two, block_inverse):
    _, slots, prim, width = assembly.shape
    rows = level_two.shape[1]
    block = block_inverse.shape[2]
    local = slots * prim
    quota = residual.shape[0]
    rhs = quota * no
    chunks = rhs // LANES
    nblk = width // block
    per = rows // block
    half = block // 2
    wide, _, slab = piece_dims(local, quota)
    packed = pl.cdiv(rows + per, LANES) * LANES
    kinds = 6 if ns == 4 else ns - 1
    vmem = pl.BlockSpec(memory_space=pltpu.VMEM)
    anywhere = pl.BlockSpec(memory_space=pl.ANY)
    dma = pltpu.SemaphoreType.DMA
    dims = (no, ns, rows, width, block, local, rhs)
    return pl.pallas_call(
        functools.partial(kernel, dims),
        out_shape=(pltpu.VMEM(residual.shape, F32), pltpu.VMEM((1, rows, rhs), F32)),
        in_specs=[anywhere, pl.BlockSpec(memory_space=pltpu.SMEM)] + [anywhere] * 3,
        out_specs=(vmem, vmem),
        scratch_shapes=[
            pltpu.VMEM(residual.shape, F32),
            pltpu.VMEM((rows, width), F32),
            pltpu.VMEM((rows, width), BF16),
            pltpu.VMEM((rows, width), BF16),
            pltpu.VMEM((chunks, width, 2 * LANES), BF16),
            pltpu.VMEM((chunks, width, LANES), F32),
            pltpu.VMEM((chunks, rows, LANES), F32),
            pltpu.VMEM((chunks, rows, LANES), F32),
            pltpu.VMEM((ITERS - 1, chunks, width, LANES), F32),
            pltpu.VMEM((chunks, rows, LANES), F32),
            pltpu.VMEM((block, rows), F32),
            pltpu.VMEM((ns * half, packed), F32),
            pltpu.VMEM((nblk, block, block), BF16),
            pltpu.VMEM((nblk, block, block), BF16),
            pltpu.VMEM((ns * 8, local), F32),
            pltpu.VMEM((no * slab, wide), F32),
            pltpu.VMEM((no * slab, wide), F32),
            pltpu.VMEM((chunks, ns * local, LANES), F32),
            pltpu.VMEM((local, 2 * LANES), BF16),
            pltpu.VMEM((ns, width, local), BF16),
            pltpu.VMEM((local, width), BF16),
            pltpu.VMEM((chunks, local, LANES), F32),
            pltpu.VMEM((chunks, local, LANES), F32),
            pltpu.VMEM((ITERS, chunks, ns * 8, LANES), F32),
            pltpu.VMEM((no * slab, wide), F32),
            pltpu.VMEM((no * slab, wide), F32),
            pltpu.VMEM((prim, slots, width), jnp.int32),
            pltpu.VMEM((local, LANES), F32),
            dma,
            dma,
            dma,
            dma,
            dma((1 + ITERS * chunks, kinds)),
            dma((1 + ITERS * chunks, kinds)),
            dma((1 + ITERS * chunks, ns - 1)),
            dma((1 + ITERS * chunks, ns - 1)),
            dma((2, no)),
            dma((2, no)),
        ],
        compiler_params=pltpu.CompilerParams(
            collective_id=0, has_side_effects=True, vmem_limit_bytes=60 * 1024 * 1024
        ),
    )(
        residual,
        counts,
        jnp.swapaxes(assembly, 1, 2),
        jnp.swapaxes(block_inverse, 1, 2),
        level_two,
    )


def solution(mesh):
    in_specs = (
        P("owner", "sub"),
        P("owner", "sub"),
        P("owner", "sub", None, None),
        P("owner", "sub", None),
        P("owner", "sub", None),
    )
    out_specs = (P("owner", "sub"), P("owner", "sub", None))
    body = functools.partial(shards, mesh.shape["owner"], mesh.shape["sub"])
    return jax.shard_map(body, mesh=mesh, in_specs=in_specs, out_specs=out_specs, check_vma=False)
```

```python
import functools

import jax
import jax.numpy as jnp
from jax import lax
from jax.experimental import pallas as pl
from jax.experimental.pallas import tpu as pltpu
from jax.sharding import PartitionSpec as P

ITERS = 4
LANES = 128
MESH = pl.DeviceIdType.MESH
F32 = jnp.float32
BF16 = jnp.bfloat16


def split(value):
    high = value.astype(BF16)
    return high, (value - high.astype(F32)).astype(BF16)


def split_cat(value):
    return jnp.concatenate(split(value), axis=1)


def fold(value):
    return value[:, :LANES] + value[:, LANES:]


def rows8(value):
    return jnp.sum(value.reshape(value.shape[0] // 8, 8, value.shape[1]), axis=0)


def dot(left, right):
    return jnp.dot(left, right, preferred_element_type=F32)


def total(acc):
    return jnp.sum(acc, axis=0, keepdims=True)


def iota(shape, axis):
    return lax.broadcasted_iota(jnp.int32, shape, axis)


def chunk_owners(chunks, parts, c):
    if chunks != 2 or parts % 2:
        return list(range(c * parts, (c + 1) * parts))
    side = parts // 2
    return [t * side + u for t in ((0, 2), (3, 1))[c] for u in range(side)]


def piece_dims(local, quota):
    wide = local - local % LANES
    rest = local % LANES
    return wide, rest, quota + (8 if rest else 0)


def kernel(
    dims,
    res_hbm,
    counts_ref,
    hot_hbm,
    inv_hbm,
    mat_hbm,
    corr_out,
    resid_out,
    res,
    mat,
    mat_hi,
    mat_lo,
    zcat,
    rvec,
    zloc,
    ploc,
    wbuf,
    wlast,
    inv_own,
    inv_pack,
    inv_hi,
    inv_lo,
    tbuf,
    send_pieces,
    recv_pieces,
    lbuf,
    lcat,
    hotmat,
    pick,
    ypick,
    corr,
    pw_buf,
    corr_pieces,
    corr_back,
    hot_own,
    tcol,
    res_sem,
    mat_sem,
    inv_sem,
    hot_sem,
    sub_send,
    sub_recv,
    small_send,
    small_recv,
    own_send,
    own_recv,
):
    no, ns, rows, width, block, local, rhs = dims
    chunks = rhs // LANES
    nblk = width // block
    per = rows // block
    quota = rhs // no
    half = block // 2
    wide, rest, slab = piece_dims(local, quota)
    parts = LANES // quota
    mo = lax.axis_index("owner")
    me = lax.axis_index("sub")
    relay = ns == 4
    xn = me + 1 - 2 * lax.rem(me, 2)
    yn = lax.rem(me + 2, ns)
    far = 3 - me
    pending = []

    def at(ref, start, size):
        return ref.at[pl.ds(pl.multiple_of(start, 8), size)]

    def span(start, size):
        return pl.ds(pl.multiple_of(start, 8), size)

    def remote(src, dst, ssem, rsem, where):
        return pltpu.make_async_remote_copy(
            src_ref=src, dst_ref=dst, send_sem=ssem, recv_sem=rsem, device_id=where,
            device_id_type=MESH,
        )

    res_copy = pltpu.make_async_copy(res_hbm, res, res_sem)
    hot_copy = pltpu.make_async_copy(hot_hbm.at[0], hot_own, hot_sem)
    inv_copy = pltpu.make_async_copy(inv_hbm.at[0], inv_own, inv_sem)
    mat_copy = pltpu.make_async_copy(mat_hbm.at[0], mat, mat_sem)
    res_copy.start()
    hot_copy.start()
    inv_copy.start()
    mat_copy.start()

    barrier = pltpu.get_barrier_semaphore()
    for step in range(1, ns):
        pl.semaphore_signal(
            barrier, inc=1, device_id={"sub": lax.rem(me + step, ns)}, device_id_type=MESH
        )
    for step in range(1, no):
        pl.semaphore_signal(
            barrier, inc=1, device_id={"owner": lax.rem(mo + step, no)}, device_id_type=MESH
        )

    class Gather:
        def __init__(self, index, buf, size):
            self.index, self.buf, self.size = index, buf, size
            self.cut = (size // 2 + 7) // 8 * 8
            self.copies = {}
            self.sent_on = False

        def part(self, who, part):
            if part == 0:
                return at(self.buf, who * self.size, self.cut)
            return at(self.buf, who * self.size + self.cut, self.size - self.cut)

        def add(self, kind, piece, peer):
            copy = remote(
                piece, piece, sub_send.at[self.index, kind], sub_recv.at[self.index, kind],
                {"sub": peer},
            )
            copy.start()
            self.copies[kind] = copy
            pending.append(copy)

        def start_part(self, part):
            for kind in ((0, 3), (1, 2))[part]:
                self.add(kind, self.part(me, part), xn if kind in (0, 2) else yn)

        def start(self):
            if relay:
                for kind, (peer, part) in enumerate(((xn, 0), (yn, 1), (xn, 1), (yn, 0))):
                    self.add(kind, self.part(me, part), peer)
            else:
                mine = at(self.buf, me * self.size, self.size)
                for step in range(1, ns):
                    self.add(step - 1, mine, lax.rem(me + step, ns))

        def forward(self):
            if relay and not self.sent_on:
                self.copies[0].wait_recv()
                self.add(4, self.part(xn, 0), yn)
                self.copies[1].wait_recv()
                self.add(5, self.part(yn, 1), xn)
            self.sent_on = True

        def pieces(self):
            size, cut = self.size, self.cut
            if relay:
                return [
                    (None, xn * size, cut),
                    (None, yn * size + cut, size - cut),
                    (self.copies[2], xn * size + cut, size - cut),
                    (self.copies[3], yn * size, cut),
                    (self.copies[4], far * size, cut),
                    (self.copies[5], far * size + cut, size - cut),
                ]
            return [
                (self.copies[step - 1], lax.rem(me + ns - step, ns) * size, size)
                for step in range(1, ns)
            ]

        def runs(self):
            kinds = ((2,), (3,), (4, 5)) if relay else [(step - 1,) for step in range(1, ns)]
            peers = (xn, yn, far) if relay else [lax.rem(me + ns - step, ns) for step in range(1, ns)]
            return list(zip(peers, kinds))

        def finish(self, kinds):
            for kind in kinds:
                self.copies[kind].wait_recv()

    def small_gather(index, buf, size):
        copies = []
        for step in range(1, ns):
            mine = at(buf, me * size, size)
            copy = remote(
                mine, mine, small_send.at[index, step - 1], small_recv.at[index, step - 1],
                {"sub": lax.rem(me + step, ns)},
            )
            copy.start()
            copies.append(copy)
            pending.append(copy)
        return copies

    def owner_copy(index, src, dst, peer):
        return remote(
            at(src, peer * slab, slab), at(dst, mo * slab, slab),
            own_send.at[index, peer], own_recv.at[index, mo], {"owner": peer},
        )

    def owner_wait(index, dst, peer):
        @pl.when(mo != peer)
        def _():
            piece = at(dst, peer * slab, slab)
            remote(
                piece, piece, own_send.at[index, peer], own_recv.at[index, peer],
                {"owner": peer},
            ).wait_recv()

    res_copy.wait()
    for part in range(no):
        low = part * local
        send_pieces[part * slab : part * slab + quota, :] = res[:, low : low + wide]
        if rest:
            strips = [
                res[t : t + 8, low + wide : low + local] for t in range(0, quota, 8)
            ]
            strips.append(jnp.zeros((8, wide - rest * len(strips)), F32))
            send_pieces[part * slab + quota : (part + 1) * slab, :] = jnp.concatenate(
                strips, axis=1
            )

    hot_copy.wait()
    prim, slots = hot_own.shape[0], hot_own.shape[1]
    for q in range(slots):
        acc = jnp.zeros((prim, LANES), F32)
        spot = iota((prim, LANES), 1)
        for lane in range(0, width, LANES):
            acc += (hot_own[:, q, lane : lane + LANES] * (spot + lane)).astype(F32)
        value = jnp.sum(acc, axis=1, keepdims=True)
        alive = iota((prim, 1), 0) < counts_ref[0, q]
        tcol[q * prim : (q + 1) * prim, :] = jnp.broadcast_to(
            jnp.where(alive, value, -1.0), (prim, LANES)
        )
    tbuf[span(me * 8, 8), :] = tcol[...].T[:8, :]

    inv_copy.wait()
    prow, pcol = iota((half, block), 0), iota((half, block), 1)
    segments, diagonals = [], []
    for q in range(per):
        top = inv_own[:half, q * block : (q + 1) * block]
        last = jnp.concatenate(
            [
                inv_own[half:block, q * block + half : (q + 1) * block],
                jnp.zeros((half, block - half), F32),
            ],
            axis=1,
        )
        segments.append(jnp.where(pcol >= prow, top, last))
        diagonals.append(jnp.sum(jnp.where(pcol == prow, last, 0.0), axis=1, keepdims=True))
    pad = inv_pack.shape[1] - rows - per
    inv_pack[span(me * half, half), :] = jnp.concatenate(
        segments + diagonals + [jnp.zeros((half, pad), F32)], axis=1
    )
    pl.semaphore_wait(barrier, ns - 1 + no - 1)

    targets = small_gather(0, tbuf, 8)
    routed = [
        owner_copy(0, send_pieces, recv_pieces, lax.rem(mo + step, no)) for step in range(1, no)
    ]
    pending.extend(routed)
    mixed = chunks == 2 and parts % 2 == 0
    early_owner = lax.rem(mo // (parts // 2), 2) == 0 if mixed else mo >= 0

    @pl.when(early_owner)
    def _():
        for copy in routed:
            copy.start()

    recv_pieces[span(mo * slab, slab), :] = send_pieces[span(mo * slab, slab), :]

    inv_gather = Gather(0, inv_pack, half)
    inv_gather.start()

    mat_copy.wait()
    strip = 48

    @pl.loop(0, rows // strip)
    def _(t):
        here = span(t * strip, strip)
        high, low = split(mat[here, :])
        mat_hi[here, :] = high
        mat_lo[here, :] = low

    @pl.when(jnp.logical_not(early_owner))
    def _():
        for copy in routed:
            copy.start()

    def arrange(c):
        owners = chunk_owners(chunks, parts, c)
        for o in owners:
            owner_wait(0, recv_pieces, o)
        body = jnp.concatenate(
            [recv_pieces[o * slab : o * slab + quota, :] for o in owners], axis=0
        )
        lbuf[c, span(me * local, wide), :] = body.T
        if rest:
            ends = jnp.concatenate(
                [
                    recv_pieces[o * slab + quota : (o + 1) * slab, t * rest : (t + 1) * rest]
                    for o in owners
                    for t in range(quota // 8)
                ],
                axis=0,
            )
            lbuf[c, span(me * local + wide, rest), :] = ends.T
        return Gather(1 + c, lbuf.at[c], local)

    def unpack(s):
        packed = inv_pack.at[span(s * half, half)]
        brow, bcol = iota((block, block), 0), iota((block, block), 1)
        for q in range(per):
            segment = packed[:, q * block : (q + 1) * block]
            ends = packed[:, rows + q : rows + q + 1]
            top = jnp.where(pcol >= prow, segment, 0.0)
            last = jnp.where(pcol < prow, segment, jnp.where(pcol == prow, ends, 0.0))
            low = jnp.concatenate(
                [jnp.zeros((half, half), F32), last[:, : block - half]], axis=1
            )
            one = jnp.concatenate([top, low], axis=0)
            high, low = split(jnp.where(brow == bcol, one, one + one.T))
            inv_hi[s * per + q] = high
            inv_lo[s * per + q] = low

    def seed(c, s, fresh):
        lcat[...] = split_cat(lbuf[c, span(s * local, local), :])

        @pl.loop(0, ns)
        def _(t):
            here = span(t * rows, rows)
            value = fold(dot(hotmat[s, here, :], lcat[...]))
            rvec[c, here, :] = value if fresh else rvec[c, here, :] + value

    unpack(me)
    for lane in range(0, width, 2 * LANES):
        spot = iota((local, 2 * LANES), 1).astype(F32) + float(lane)
        pick[:, lane : lane + 2 * LANES] = jnp.where(spot == tcol[:, :1], 1.0, 0.0).astype(BF16)

    local_gathers = [arrange(0)]
    local_gathers[0].start()
    inv_gather.forward()
    for copy in targets:
        copy.wait_recv()

    @pl.loop(0, ns)
    def _(s):
        goal = tbuf[span(s * 8, 8), :][:1, :]
        for row in range(0, width, block):
            spot = (iota((block, local), 0) + row).astype(F32)
            hotmat[s, row : row + block, :] = jnp.where(spot == goal, 1.0, 0.0).astype(BF16)

    seed(0, me, True)
    inv_runs = inv_gather.runs()
    if relay:
        s, kinds = inv_runs[0]
        inv_gather.finish(kinds)
        unpack(s)
    local_gathers[0].forward()
    if relay:
        s, kinds = inv_runs[1]
        inv_gather.finish(kinds)
        unpack(s)
    for c in range(1, chunks):
        local_gathers.append(arrange(c))
        local_gathers[c].start()
    for s, kinds in local_gathers[0].runs()[:-1]:
        local_gathers[0].finish(kinds)
        seed(0, s, False)
    if relay:
        s, kinds = inv_runs[2]
        inv_gather.finish(kinds)
        unpack(s)
    else:
        for s, kinds in inv_runs:
            inv_gather.finish(kinds)

        @pl.loop(1, ns)
        def _(t):
            unpack(lax.rem(me + t, ns))

    def precond(b, resid):
        rcat = split_cat(resid)
        return fold(dot(inv_hi[b], rcat) + dot(inv_lo[b], rcat))

    def first(c):
        last, kinds = local_gathers[c].runs()[-1]
        local_gathers[c].finish(kinds)
        lcat[...] = split_cat(lbuf[c, span(last * local, local), :])

        def run(s, acc, own):
            value = fold(dot(hotmat[last, span(s * rows, rows), :], lcat[...]))
            value = rvec[c, span(s * rows, rows), :] + value
            rvec[c, span(s * rows, rows), :] = value
            for q in range(per):
                resid = value[q * block : (q + 1) * block, :]
                z = precond(s * per + q, resid)
                zcat[c, span(s * rows + q * block, block), :] = split_cat(z)
                if own:
                    zloc[c, q * block : (q + 1) * block, :] = z
                acc = acc + rows8(resid * z)
            return acc

        acc = run(me, jnp.zeros((8, LANES), F32), True)
        return total(
            lax.fori_loop(1, ns, lambda t, acc: run(lax.rem(me + t, ns), acc, False), acc)
        )

    def update(k, c, gather, sums, rz):
        for copy in sums:
            copy.wait_recv()
        alpha = rz / total(rows8(pw_buf[k, c]))
        corr[c] = alpha * ypick[c] + (corr[c] if k else 0.0)

        def one(b):
            here = span(b * block, block)
            resid = rvec[c, here, :] - alpha * wbuf[k, c, here, :]
            rvec[c, here, :] = resid
            z = precond(b, resid)
            zcat[c, here, :] = split_cat(z)
            return z, rows8(resid * z)

        acc = jnp.zeros((8, LANES), F32)
        for q in range(per):
            z, part = one(me * per + q)
            zloc[c, q * block : (q + 1) * block, :] = z
            acc = acc + part
        gather.forward()
        for copy, start, size in gather.pieces():
            if copy is not None:
                copy.wait_recv()
            for u in range(size // block):
                acc = acc + one(start // block + u)[1]
        rz_next = total(acc)
        return rz_next, rz_next / rz

    tile = 2 * block if rows % (2 * block) == 0 else block

    def image(k, c, beta, gather=None):
        def body(t, acc):
            here = span(t * tile, tile)
            there = span(me * rows + t * tile, tile)
            w = fold(dot(mat_hi[here, :], zcat[c]) + dot(mat_lo[here, :], zcat[c]))
            p = zloc[c, here, :]
            if k:
                w = w + beta * wbuf[k - 1, c, there, :]
                p = p + beta * ploc[c, here, :]
            ploc[c, here, :] = p
            if k < ITERS - 1:
                wbuf[k, c, there, :] = w
            else:
                wlast[c, here, :] = w
            return acc + rows8(p * w)

        acc = jnp.zeros((8, LANES), F32)
        if gather is None:
            acc = lax.fori_loop(0, rows // tile, body, acc)
        else:
            for part in range(2):
                acc = body(part, acc)
                gather.start_part(part)
        pw_buf[k, c, span(me * 8, 8), :] = acc
        return small_gather(1 + k * chunks + c, pw_buf.at[k, c], 8)

    def rows_gather(k, c):
        return Gather(1 + chunks + k * chunks + c, wbuf.at[k, c], rows)

    def spread(k, c, earlier):
        earlier.forward()
        gather = rows_gather(k, c)
        gather.start()
        return gather

    def picked(k, c, beta):
        y = fold(dot(pick[...], zcat[c]))
        ypick[c] = y + beta * ypick[c] if k else y

    def conclude(c, sums, rz):
        for copy in sums:
            copy.wait_recv()
        alpha = rz / total(rows8(pw_buf[ITERS - 1, c]))
        value = corr[c] + alpha * ypick[c]
        owners = chunk_owners(chunks, parts, c)
        body = value[:wide, :].T
        ends = value[wide:, :].T if rest else None
        for t, o in enumerate(owners):
            low = t * quota
            corr_pieces[o * slab : o * slab + quota, :] = body[low : low + quota, :]
            if rest:
                strips = [ends[low + t : low + t + 8, :] for t in range(0, quota, 8)]
                strips.append(jnp.zeros((8, wide - rest * len(strips)), F32))
                corr_pieces[o * slab + quota : (o + 1) * slab, :] = jnp.concatenate(
                    strips, axis=1
                )
        for o in owners:
            @pl.when(mo != o)
            def _(o=o):
                owner_copy(1, corr_pieces, corr_back, o).start()
        left = rvec[c, span(me * rows, rows), :] - alpha * wlast[c]
        if not mixed:
            resid_out[0, :, c * LANES : (c + 1) * LANES] = left
        elif c == 0:
            wlast[c] = left
        else:
            side = iota(left.shape, 1) < LANES // 2
            resid_out[0, :, :LANES] = jnp.where(side, wlast[0], left)
            resid_out[0, :, LANES:] = pltpu.roll(jnp.where(side, left, wlast[0]), LANES // 2, 1)

    rz, beta = [None] * chunks, [None] * chunks
    sums, flight, earlier = [None] * chunks, [None] * chunks, None
    for c in range(chunks):
        if c:
            seed(c, me, True)
            for s, kinds in local_gathers[c].runs()[:-1]:
                local_gathers[c].finish(kinds)
                seed(c, s, False)
        rz[c] = first(c)
        if c == 0:
            for gather in local_gathers[1:]:
                gather.forward()
        if c:
            earlier.forward()
            sums[c] = image(0, c, None)
            earlier = flight[c] = spread(0, c, earlier)
        else:
            earlier = flight[c] = rows_gather(0, c)
            early = relay and tile * 2 == rows and tile == earlier.cut
            sums[c] = image(0, c, None, earlier if early else None)
            if not early:
                earlier.start()
    for c in range(chunks):
        picked(0, c, None)

    for k in range(ITERS - 1):
        final = k == ITERS - 2
        for c in range(chunks):
            if final and c:
                earlier.forward()
            rz[c], beta[c] = update(k, c, flight[c], sums[c], rz[c])
            sums[c] = image(k + 1, c, beta[c])
            if not final:
                earlier = flight[c] = spread(k + 1, c, earlier)
            picked(k + 1, c, beta[c])
    for c in range(chunks):
        conclude(c, sums[c], rz[c])

    corr_back[span(mo * slab, slab), :] = corr_pieces[span(mo * slab, slab), :]
    for part in range(no):
        owner_wait(1, corr_back, part)
        low = part * local
        corr_out[:, low : low + wide] = corr_back[part * slab : part * slab + quota, :]
        for t in range(quota // 8 if rest else 0):
            corr_out[8 * t : 8 * t + 8, low + wide : low + local] = corr_back[
                part * slab + quota : (part + 1) * slab, t * rest : (t + 1) * rest
            ]
    for copy in pending:
        copy.wait_send()
    for o in range(no):
        @pl.when(mo != o)
        def _(o=o):
            owner_copy(1, corr_pieces, corr_back, o).wait_send()


def shards(no, ns, residual, counts, assembly, level_two, block_inverse):
    _, slots, prim, width = assembly.shape
    rows = level_two.shape[1]
    block = block_inverse.shape[2]
    local = slots * prim
    quota = residual.shape[0]
    rhs = quota * no
    chunks = rhs // LANES
    nblk = width // block
    per = rows // block
    half = block // 2
    wide, _, slab = piece_dims(local, quota)
    packed = pl.cdiv(rows + per, LANES) * LANES
    kinds = 6 if ns == 4 else ns - 1
    vmem = pl.BlockSpec(memory_space=pltpu.VMEM)
    anywhere = pl.BlockSpec(memory_space=pl.ANY)
    dma = pltpu.SemaphoreType.DMA
    dims = (no, ns, rows, width, block, local, rhs)
    return pl.pallas_call(
        functools.partial(kernel, dims),
        out_shape=(pltpu.VMEM(residual.shape, F32), pltpu.VMEM((1, rows, rhs), F32)),
        in_specs=[anywhere, pl.BlockSpec(memory_space=pltpu.SMEM)] + [anywhere] * 3,
        out_specs=(vmem, vmem),
        scratch_shapes=[
            pltpu.VMEM(residual.shape, F32),
            pltpu.VMEM((rows, width), F32),
            pltpu.VMEM((rows, width), BF16),
            pltpu.VMEM((rows, width), BF16),
            pltpu.VMEM((chunks, width, 2 * LANES), BF16),
            pltpu.VMEM((chunks, width, LANES), F32),
            pltpu.VMEM((chunks, rows, LANES), F32),
            pltpu.VMEM((chunks, rows, LANES), F32),
            pltpu.VMEM((ITERS - 1, chunks, width, LANES), F32),
            pltpu.VMEM((chunks, rows, LANES), F32),
            pltpu.VMEM((block, rows), F32),
            pltpu.VMEM((ns * half, packed), F32),
            pltpu.VMEM((nblk, block, block), BF16),
            pltpu.VMEM((nblk, block, block), BF16),
            pltpu.VMEM((ns * 8, local), F32),
            pltpu.VMEM((no * slab, wide), F32),
            pltpu.VMEM((no * slab, wide), F32),
            pltpu.VMEM((chunks, ns * local, LANES), F32),
            pltpu.VMEM((local, 2 * LANES), BF16),
            pltpu.VMEM((ns, width, local), BF16),
            pltpu.VMEM((local, width), BF16),
            pltpu.VMEM((chunks, local, LANES), F32),
            pltpu.VMEM((chunks, local, LANES), F32),
            pltpu.VMEM((ITERS, chunks, ns * 8, LANES), F32),
            pltpu.VMEM((no * slab, wide), F32),
            pltpu.VMEM((no * slab, wide), F32),
            pltpu.VMEM((prim, slots, width), jnp.int32),
            pltpu.VMEM((local, LANES), F32),
            dma,
            dma,
            dma,
            dma,
            dma((1 + ITERS * chunks, kinds)),
            dma((1 + ITERS * chunks, kinds)),
            dma((1 + ITERS * chunks, ns - 1)),
            dma((1 + ITERS * chunks, ns - 1)),
            dma((2, no)),
            dma((2, no)),
        ],
        compiler_params=pltpu.CompilerParams(
            collective_id=0, has_side_effects=True, vmem_limit_bytes=60 * 1024 * 1024
        ),
    )(
        residual,
        counts,
        jnp.swapaxes(assembly, 1, 2),
        jnp.swapaxes(block_inverse, 1, 2),
        level_two,
    )


def solution(mesh):
    in_specs = (
        P("owner", "sub"),
        P("owner", "sub"),
        P("owner", "sub", None, None),
        P("owner", "sub", None),
        P("owner", "sub", None),
    )
    out_specs = (P("owner", "sub"), P("owner", "sub", None))
    body = functools.partial(shards, mesh.shape["owner"], mesh.shape["sub"])
    return jax.shard_map(body, mesh=mesh, in_specs=in_specs, out_specs=out_specs, check_vma=False)
```
